32 devices in a mesh: dp: 8 (over y, x, core), mp: 4 (over z).
Axes of the slice: x: 2, y: 2, z: 4, core: 2. Of those that a mesh axis runs over, the one named last changes fastest.
Arguments:
- hidden_rows: bfloat16 [4096, 3584], P('dp'), may hold values from -6 to 6
- key_grad: bfloat16 [4096, 512], P('dp', 'mp'), may hold values from -6 to 6
- value_grad: bfloat16 [4096, 512], P('dp', 'mp'), may hold values from -6 to 6
- visual_rows: bfloat16 [2048, 1024], P('dp'), may hold values from -6 to 6
- visual_cotangent: bfloat16 [8, 4, 64, 3584], P('dp'), may hold values from -6 to 6
- norm_gain: float32 [1024], replicated, may hold values from 0.25 to 1.75
- norm_bias: float32 [1024], replicated, may hold values from -3 to 3
- fc1_weight: bfloat16 [1024, 4096], P(None, 'mp'), may hold values from -0.1875 to 0.1875
- fc1_bias: float32 [4096], P('mp'), may hold values from -3 to 3
- fc2_weight: bfloat16 [4096, 1024], P('mp'), may hold values from -0.09375 to 0.09375
- fc2_bias: float32 [1024], replicated, may hold values from -3 to 3
- layer_scale: float32 [1024], replicated, may hold values from 0.3 to 1.5
- token_counts: int32 [8, 8], P('dp'), may hold values from 1 to 32, as said below
- dest_offsets: int32 [8, 8], P('dp'), may hold values from 1 to 4, as said below
Outputs:
- key_weight_grad: float32 [3592, 512], P('dp', 'mp')
- value_weight_grad: float32 [3592, 512], P('dp', 'mp')
- projector_grad: float32 [3592, 1024], P('dp', 'mp')
- handoff: bfloat16 [8, 4, 64, 1024], P('dp', None, None, 'mp')
The draws below stay inside these ranges and needn't reach their ends.
Inputs may be any that keep to these rules, and one draw needn't show every extreme that they name: `token_counts`: on every data rank the images of one distance, chosen per rank, all have 32 rows. `dest_offsets`: every data rank sends exactly 2 images to each distance from 1 to 4.
All inputs are finite; a program needn't handle non-finite values.
Results may differ from the reference program's by a relative error of at most 0.0046.
Values may be sent and summed in bfloat16 or wider, within the bound.
A program may use at most 64 MiB of HBM per device.

```python
import math
import jax
import jax.numpy as jnp
from jax import lax

D = 3584
KV_WIDTH = 512
FEAT = 1024
MLP = 4096
TOK_DEV = 512
MOST_TOK = 32
SPREAD = 4
IMG_DEV = 8
ROWS_DEV = 256
CAP = 64
TOKENS = 4096
D_PAD = 3592
N_DP = 8


def routing_table(key):
    base = jax.random.fold_in(key, 11)
    source_keys = jax.random.split(base, N_DP)

    def one_source(source_key):
        first, second, third = jax.random.split(source_key, 3)
        order = jax.random.permutation(first, IMG_DEV)
        offsets = (order % SPREAD + 1).astype(jnp.int32)
        counts = jax.random.randint(second, (IMG_DEV,), 1, MOST_TOK + 1).astype(jnp.int32)
        filled = jax.random.randint(third, (), 1, SPREAD + 1).astype(jnp.int32)
        counts = jnp.where(offsets == filled, MOST_TOK, counts).astype(jnp.int32)
        return (counts, offsets)
    return jax.vmap(one_source)(source_keys)


def draw_token_counts(key, part):
    return routing_table(key)[0]


def draw_dest_offsets(key, part):
    return routing_table(key)[1]


def strengthened(values, own_key, source, target, shards_of, factor):
    owner, partner = [(jnp.arange(values.shape[dim]) // (values.shape[dim] // shards_of)).reshape([-1 if axis == dim else 1 for axis in range(values.ndim)]) for dim in (source, target)]
    chosen = jax.random.permutation(own_key, shards_of)[partner]
    strong = (owner == chosen) | (owner == (partner + shards_of // 2) % shards_of)
    return jnp.where(strong, factor * values, values)


def block_levels(key, shape, shards, smallest, high):
    loudness = 1.0
    for dim, blocks in shards:
        draws = jax.random.uniform(jax.random.fold_in(jax.random.fold_in(key, 6), dim), (blocks,), jnp.float32, smallest / len(shards), high / len(shards))
        loudness = loudness * jnp.repeat(jnp.exp(draws), shape[dim] // blocks).reshape((-1,) + (1,) * (len(shape) - 1 - dim))
    return loudness


def noise(own_key, shape, scale, reach, cuts=(), dtype=jnp.bfloat16):
    result = scale * jax.random.normal(own_key, shape, jnp.float32)
    if cuts:
        result = result * block_levels(own_key, shape, cuts, -0.22, 0.18)
    return jnp.clip(result, -reach, reach).astype(dtype)


def noise_with(stream_key, shape, spread, bound, cuts, heavy, dtype=jnp.bfloat16):
    entries = spread * jax.random.normal(stream_key, shape, jnp.float32)
    if cuts:
        entries = entries * block_levels(stream_key, shape, cuts, -0.22, 0.18)
    return jnp.clip(strengthened(entries, jax.random.fold_in(stream_key, 3), *heavy), -bound, bound).astype(dtype)


def setup_inputs(seed: int = 0) -> dict:
    keys = jax.random.split(jax.random.key(seed), 15)
    return {
        "hidden_rows": noise_with(keys[0], (TOKENS, D), 1.0, 6.0, ((0, 8),), (0, 1, 8, 2.0)),
        "key_grad": noise(keys[1], (TOKENS, KV_WIDTH), 1.0, 6.0, ((0, 8), (1, 4))),
        "value_grad": noise(keys[2], (TOKENS, KV_WIDTH), 1.0, 6.0, ((0, 8), (1, 4))),
        "visual_rows": noise(keys[3], (N_DP * ROWS_DEV, FEAT), 1.0, 6.0, ((0, 8),)),
        "visual_cotangent": noise_with(keys[4], (N_DP, SPREAD, CAP, D), 1.0, 6.0, ((0, 8),), (0, 3, 8, 2.0)),
        "norm_gain": jnp.clip(1.0 + 0.15 * jax.random.normal(keys[5], (FEAT,), jnp.float32), 0.25, 1.75),
        "norm_bias": noise(keys[6], (FEAT,), 0.5, 3.0, (), jnp.float32),
        "fc1_weight": noise(keys[7], (FEAT, MLP), FEAT ** -0.5, 0.1875, ((1, 4),)),
        "fc1_bias": noise(keys[8], (MLP,), 0.5, 3.0, ((0, 4),), jnp.float32),
        "fc2_weight": noise(keys[9], (MLP, FEAT), MLP ** -0.5, 0.09375, ((0, 4),)),
        "fc2_bias": noise(keys[10], (FEAT,), 0.5, 3.0, (), jnp.float32),
        "layer_scale": jnp.clip(jnp.exp(jax.random.uniform(keys[11], (FEAT,), jnp.float32, math.log(0.3), math.log(1.5))), 0.3, 1.5),
        "token_counts": draw_token_counts(jax.random.fold_in(keys[14], 71), 0),
        "dest_offsets": draw_dest_offsets(jax.random.fold_in(keys[14], 71), 0),
    }


def pack_rows(rows, counts, offsets):
    total_rows = rows.shape[0]
    images = counts.shape[0]
    counts = counts.astype(jnp.int32)
    offsets = offsets.astype(jnp.int32)
    ends = jnp.cumsum(counts).astype(jnp.int32)
    starts = (ends - counts).astype(jnp.int32)
    places = jnp.arange(total_rows).astype(jnp.int32)
    image_ids = jnp.arange(images).astype(jnp.int32)
    owner = lax.optimization_barrier(jnp.sum((places[:, None] >= ends[None, :]).astype(jnp.int32), axis=1)).astype(jnp.int32)
    member = (owner[:, None] == image_ids[None, :]).astype(jnp.int32)
    earlier = (image_ids[None, :] < image_ids[:, None]) & (offsets[None, :] == offsets[:, None])
    before = lax.optimization_barrier(jnp.sum(earlier.astype(jnp.int32) * counts[None, :], axis=1)).astype(jnp.int32)
    row_dest = lax.optimization_barrier(jnp.sum(member * offsets[None, :], axis=1)).astype(jnp.int32)
    row_start = lax.optimization_barrier(jnp.sum(member * starts[None, :], axis=1)).astype(jnp.int32)
    row_before = lax.optimization_barrier(jnp.sum(member * before[None, :], axis=1)).astype(jnp.int32)
    slot_index = row_before + places - row_start
    target = jnp.where(places < ends[images - 1], (row_dest - 1) * CAP + slot_index, -1).astype(jnp.int32)
    slot_ids = jnp.arange(SPREAD * CAP).astype(jnp.int32)
    select = (slot_ids[:, None] == target[None, :]).astype(jnp.bfloat16)
    packed = jnp.dot(select, rows, preferred_element_type=jnp.float32).astype(jnp.bfloat16)
    return packed.reshape(SPREAD, CAP, rows.shape[1])

def encode(rows, norm_gain, norm_bias, fc1_weight, fc1_bias, fc2_weight, fc2_bias, layer_scale):
    values = rows.astype(jnp.float32)
    center = lax.optimization_barrier(jnp.mean(values, axis=1, keepdims=True))
    spread_sq = lax.optimization_barrier(jnp.mean((values - center) ** 2, axis=1, keepdims=True))
    normed = ((values - center) * lax.rsqrt(spread_sq + 1e-06) * norm_gain + norm_bias).astype(jnp.bfloat16)
    hidden = jax.nn.gelu(jnp.dot(normed, fc1_weight, preferred_element_type=jnp.float32) + fc1_bias, approximate=False).astype(jnp.bfloat16)
    partial_value = jnp.dot(hidden, fc2_weight, preferred_element_type=jnp.float32)
    return (values + layer_scale * (partial_value + fc2_bias)).astype(jnp.bfloat16)

def reference(hidden_rows, key_grad, value_grad, visual_rows, visual_cotangent, norm_gain, norm_bias, fc1_weight, fc1_bias, fc2_weight, fc2_bias, layer_scale, token_counts, dest_offsets):
    width = hidden_rows.shape[1]
    blocks = hidden_rows.reshape(N_DP, TOK_DEV, width)
    key_blocks = key_grad.reshape(N_DP, TOK_DEV, KV_WIDTH)
    value_blocks = value_grad.reshape(N_DP, TOK_DEV, KV_WIDTH)

    def accumulate(carry, pieces):
        inputs, key_piece, value_piece = pieces
        key_total, value_total = carry
        key_total = key_total + lax.dot_general(inputs, key_piece, (((0,), (0,)), ((), ())), preferred_element_type=jnp.float32)
        value_total = value_total + lax.dot_general(inputs, value_piece, (((0,), (0,)), ((), ())), preferred_element_type=jnp.float32)
        return ((key_total, value_total), None)
    empty = jnp.zeros((width, KV_WIDTH), jnp.float32)
    (key_total, value_total), _ = lax.scan(accumulate, (empty, empty), (blocks, key_blocks, value_blocks))
    key_bias = lax.optimization_barrier(jnp.sum(key_grad.astype(jnp.float32), axis=0))[None, :]
    value_bias = lax.optimization_barrier(jnp.sum(value_grad.astype(jnp.float32), axis=0))[None, :]
    zero_rows = jnp.zeros((D_PAD - width - 1, KV_WIDTH), jnp.float32)
    key_weight_grad = jnp.concatenate([key_total, key_bias, zero_rows], axis=0)
    value_weight_grad = jnp.concatenate([value_total, value_bias, zero_rows], axis=0)
    encoded = encode(visual_rows, norm_gain, norm_bias, fc1_weight, fc1_bias, fc2_weight, fc2_bias, layer_scale)
    packed = jax.vmap(pack_rows)(encoded.reshape(N_DP, ROWS_DEV, FEAT), token_counts, dest_offsets)
    handoff = jnp.stack([jnp.roll(packed[:, distance], distance + 1, axis=0) for distance in range(SPREAD)], axis=1)
    cot_flat = visual_cotangent.reshape(N_DP * SPREAD * CAP, width)
    rows_flat = handoff.reshape(N_DP * SPREAD * CAP, FEAT)
    projector_main = lax.dot_general(cot_flat, rows_flat, (((0,), (0,)), ((), ())), preferred_element_type=jnp.float32)
    projector_grad = jnp.concatenate([projector_main, jnp.zeros((D_PAD - width, FEAT), jnp.float32)], axis=0)
    return (key_weight_grad, value_weight_grad, projector_grad, handoff)
```

```python
import functools

import jax
import jax.numpy as jnp
from jax import lax
from jax.experimental import pallas as pl
from jax.experimental.pallas import tpu as pltpu
from jax.sharding import PartitionSpec as P

MESH = pl.DeviceIdType.MESH
BF = jnp.bfloat16
F32 = jnp.float32


def up(x, m):
    return -(-x // m) * m


def factors(n):
    core = 2 if n % 2 == 0 else 1
    rest = n // core
    inner = max(f for f in range(1, rest + 1) if rest % f == 0 and f * f <= rest)
    return core, inner, rest // inner


def erf_gelu(x):
    return 0.5 * x * (1.0 + lax.erf(x * (0.5**0.5)))


def kernel(
    cfg,
    hid_h, key_h, val_h, vis_h, cot_h, fc1_h, fc2_h,
    gain, beta, fc1_b, fc2_b, scale, counts, offsets,
    key_o, val_o, proj_o, hand_o,
    hid, key, val, vis, cot, fc1, fc2,
    big_k, big_v, big_c,
    cot_send, cot_recv,
    k0, k0r, k1, k1r, k2, k2r,
    v0, v0r, v1, v1r, v2, v2r,
    z_send, z_recv, gath,
    load_sem, cot_ss, cot_rs, z_ss, z_rs,
    k0_s, k0_r, k1_s, k1_r, k2_s, k2_r,
    v0_s, v0_r, v1_s, v1_r, v2_s, v2_r,
    g_s, g_r, f_s, f_r,
):
    n, mp, shard, rows_pad, spread, cap = cfg
    nc, na, nb = factors(n)
    me = lax.axis_index("dp")
    col = lax.axis_index("mp")
    dc = lax.rem(me, nc)
    da = lax.rem(lax.div(me, nc), na)
    db = lax.div(me, nc * na)
    tokens, width = hid.shape
    slots = cot.shape[0]
    kc = key.shape[1]
    fcol = hand_o.shape[1]

    def rank(c, a, b):
        return (b * na + a) * nc + c

    loads = []
    for i, (src, dst) in enumerate(
        ((cot_h, cot), (vis_h, vis), (fc1_h, fc1), (fc2_h, fc2), (hid_h, hid), (key_h, key), (val_h, val))
    ):
        cp = pltpu.make_async_copy(src, dst, load_sem.at[i])
        cp.start()
        loads.append(cp)
    barrier = pltpu.get_barrier_semaphore()
    for j in range(1, n):
        pl.semaphore_signal(barrier, inc=1, device_id={"dp": lax.rem(me + j, n)}, device_id_type=MESH)
    for j in range(1, mp):
        pl.semaphore_signal(barrier, inc=1, device_id={"mp": lax.rem(col + j, mp)}, device_id_type=MESH)

    def remote(src, dst, ss, rs, where):
        cp = pltpu.make_async_remote_copy(
            src_ref=src, dst_ref=dst, send_sem=ss, recv_sem=rs, device_id=where, device_id_type=MESH
        )
        cp.start()
        return cp

    step = 512 if width % 512 == 0 else 128

    loads[0].wait()
    half = 128

    def turn(i, _):
        at = pl.multiple_of(i * step, step)
        for h in range(slots // half):
            piece = cot[h * half : (h + 1) * half, pl.ds(at, step)].astype(F32)
            big_c[h, pl.ds(at, step), :] = piece.T
        return 0

    lax.fori_loop(0, width // step, turn, 0)
    tail = big_c.shape[1] - width
    big_c[:, width:, :] = jnp.zeros((slots // half, tail, half), F32)
    for r in range(n):
        for h in range(slots // half):
            cot_send[r, :, h * half : (h + 1) * half] = big_c[h, r * shard : r * shard + rows_pad, :].astype(BF)
    pl.semaphore_wait(barrier, n - 1 + mp - 1)
    cot_cps = []

    def send_cot():
        for j in range(1, n):
            to = lax.rem(me + j, n)
            cot_cps.append(remote(cot_send.at[to], cot_recv.at[j - 1], cot_ss.at[j - 1], cot_rs.at[j - 1], {"dp": to}))

    send_cot()

    loads[1].wait()
    values = vis[...].astype(F32)
    center = jnp.mean(values, axis=1, keepdims=True)
    cen = values - center
    var = jnp.mean(cen * cen, axis=1, keepdims=True)
    normed = (cen * lax.rsqrt(var + 1e-06) * gain[...] + beta[...]).astype(BF)
    loads[2].wait()
    hidden = erf_gelu(jnp.dot(normed, fc1[...], preferred_element_type=F32) + fc1_b[...]).astype(BF)
    loads[3].wait()

    def feat(i):
        return pl.ds(pl.multiple_of(i * fcol, 128), fcol)

    z_cps = []
    order = sorted(range(1, mp), key=lambda j: abs(j - mp / 2))
    for j in order:
        to = lax.rem(col + j, mp)
        z_send[j - 1] = jnp.dot(hidden, fc2[:, feat(to)], preferred_element_type=F32).astype(BF)
        z_cps.append(remote(z_send.at[j - 1], z_recv.at[j - 1], z_ss.at[j - 1], z_rs.at[j - 1], {"mp": to}))
    own = jnp.dot(hidden, fc2[:, feat(col)], preferred_element_type=F32)

    for cp in loads[4:]:
        cp.wait()
    kv = jnp.concatenate([key[...], val[...]], axis=1)

    def product(i, _):
        at = pl.multiple_of(i * step, step)
        res = lax.dot_general(hid[:, pl.ds(at, step)], kv, (((0,), (0,)), ((), ())), preferred_element_type=F32)
        big_k[pl.ds(at, step), :] = res[:, :kc]
        big_v[pl.ds(at, step), :] = res[:, kc:]
        return 0

    lax.fori_loop(0, width // step, product, 0)
    first = lax.broadcasted_iota(jnp.int32, (tail, kc), 0) == 0
    big_k[width:, :] = jnp.where(first, jnp.sum(key[...].astype(F32), axis=0, keepdims=True), 0.0)
    big_v[width:, :] = jnp.where(first, jnp.sum(val[...].astype(F32), axis=0, keepdims=True), 0.0)
    for r in range(n):
        c, a, b = r % nc, (r // nc) % na, r // (nc * na)
        k0[c, a, b] = big_k[r * shard : r * shard + rows_pad, :].astype(BF)
        v0[c, b, a] = big_v[r * shard : r * shard + rows_pad, :].astype(BF)

    def exchange(buf, got, ss, rs, digit, q, peer_of):
        cps = []
        for j in range(1, q):
            to = lax.rem(digit + j, q)
            cps.append(remote(buf.at[to], got.at[j - 1], ss.at[j - 1], rs.at[j - 1], {"dp": peer_of(to)}))
        return cps

    def added(buf, got, digit, q, at):
        total = buf[(digit,) + at].astype(F32)
        for j in range(1, q):
            total = total + got[(j - 1,) + at].astype(F32)
        return total

    at_c = lambda c: rank(c, da, db)
    at_a = lambda a: rank(dc, a, db)
    at_b = lambda b: rank(dc, da, b)
    s0k = exchange(k0, k0r, k0_s, k0_r, dc, nc, at_c)
    s0v = exchange(v0, v0r, v0_s, v0_r, dc, nc, at_c)

    rows = vis.shape[0]
    images = counts.shape[1]
    place = lax.broadcasted_iota(jnp.int32, (1, rows), 1)
    target = jnp.full((1, rows), -1, jnp.int32)
    start = jnp.int32(0)
    for i in range(images):
        cnt, off = counts[0, i], offsets[0, i]
        before = jnp.int32(0)
        for e in range(i):
            before = before + jnp.where(offsets[0, e] == off, counts[0, e], 0)
        inside = (place >= start) & (place < start + cnt)
        target = jnp.where(inside, (off - 1) * cap + before + place - start, target)
        start = start + cnt
    slot_id = lax.broadcasted_iota(jnp.int32, (spread * cap, rows), 0)
    select = jnp.where(slot_id == target, 1.0, 0.0).astype(BF)

    for cp in s0k:
        cp.wait_recv()
    for a in range(na):
        for b in range(nb):
            k1[a, b] = added(k0, k0r, dc, nc, (a, b)).astype(BF)
    s1k = exchange(k1, k1r, k1_s, k1_r, da, na, at_a)
    for cp in s0v:
        cp.wait_recv()
    for b in range(nb):
        for a in range(na):
            v1[b, a] = added(v0, v0r, dc, nc, (b, a)).astype(BF)
    s1v = exchange(v1, v1r, v1_s, v1_r, db, nb, at_b)

    for cp in z_cps:
        cp.wait_recv()
    summed = own
    for j in range(1, mp):
        summed = summed + z_recv[j - 1].astype(F32)
    encoded = (
        vis[:, feat(col)].astype(F32) + scale[:, feat(col)] * (summed + fc2_b[:, feat(col)])
    ).astype(BF)
    gath[me] = jnp.dot(select, encoded, preferred_element_type=F32).astype(BF)
    chips = n // nc
    chip = lax.div(me, nc)
    g_cps, f_cps = [], []
    for j in range(1, nc):
        f_cps.append(
            remote(gath.at[me], gath.at[me], f_s.at[0, j - 1], f_r.at[0, j - 1], {"dp": at_c(lax.rem(dc + j, nc))})
        )
    for j in range(1, chips):
        to = lax.rem(chip + j, chips) * nc + dc
        g_cps.append(remote(gath.at[me], gath.at[me], g_s.at[j - 1], g_r.at[j - 1], {"dp": to}))

    for cp in s1k:
        cp.wait_recv()
    for b in range(nb):
        k2[b] = added(k1, k1r, da, na, (b,)).astype(BF)
    s2k = exchange(k2, k2r, k2_s, k2_r, db, nb, at_b)
    for cp in s1v:
        cp.wait_recv()
    for a in range(na):
        v2[a] = added(v1, v1r, db, nb, (a,)).astype(BF)
    s2v = exchange(v2, v2r, v2_s, v2_r, da, na, at_a)

    for j in range(1, chips):
        g_cps[j - 1].wait_recv()
        source = lax.rem(chip + chips - j, chips) * nc + dc
        for i in range(1, nc):
            f_cps.append(
                remote(
                    gath.at[source], gath.at[source], f_s.at[j, i - 1], f_r.at[j, i - 1],
                    {"dp": at_c(lax.rem(dc + i, nc))},
                )
            )
    for cp in f_cps:
        cp.wait_recv()

    def received(r):
        parts = []
        for k in range(1, spread + 1):
            source = lax.rem(r + n - k, n)
            parts.append(gath[source, (k - 1) * cap : k * cap, :])
        return jnp.concatenate(parts, axis=0)

    mine = received(me)
    hand_o[...] = mine
    total = jnp.dot(cot_send[me], mine, preferred_element_type=F32)
    for j in range(1, n):
        cot_cps[j - 1].wait_recv()
        total = total + jnp.dot(
            cot_recv[j - 1], received(lax.rem(me + n - j, n)), preferred_element_type=F32
        )
    proj_o[...] = total[:shard]

    for cp in s2k:
        cp.wait_recv()
    key_o[...] = added(k2, k2r, db, nb, ())[:shard]
    for cp in s2v:
        cp.wait_recv()
    val_o[...] = added(v2, v2r, da, na, ())[:shard]
    for cp in cot_cps + z_cps + s0k + s0v + s1k + s1v + s2k + s2v + g_cps + f_cps:
        cp.wait_send()


def per_device(
    n, mp, hidden_rows, key_grad, value_grad, visual_rows, visual_cotangent, norm_gain, norm_bias,
    fc1_weight, fc1_bias, fc2_weight, fc2_bias, layer_scale, token_counts, dest_offsets,
):
    tokens, width = hidden_rows.shape
    spread, cap = visual_cotangent.shape[1:3]
    slots = spread * cap
    shard = (width + n) // n
    rp = up(shard, 16)
    nc, na, nb = factors(n)
    kc = key_grad.shape[1]
    rows, feats = visual_rows.shape
    fcol = feats // mp
    tall = up(max((n - 1) * shard + rp, width + 8), 8)
    any_spec = pl.BlockSpec(memory_space=pl.ANY)
    vm = pl.BlockSpec(memory_space=pltpu.VMEM)
    sm = pl.BlockSpec(memory_space=pltpu.SMEM)
    dma = lambda *s: pltpu.SemaphoreType.DMA(tuple(max(x, 1) for x in s))

    def stages(q1, q2):
        return [
            pltpu.VMEM((nc, q1, q2, rp, kc), BF),
            pltpu.VMEM((max(nc - 1, 1), q1, q2, rp, kc), BF),
            pltpu.VMEM((q1, q2, rp, kc), BF),
            pltpu.VMEM((max(q1 - 1, 1), q2, rp, kc), BF),
            pltpu.VMEM((q2, rp, kc), BF),
            pltpu.VMEM((max(q2 - 1, 1), rp, kc), BF),
        ]

    def stage_sems(q1, q2):
        return [dma(q - 1) for q in (nc, nc, q1, q1, q2, q2)]

    outs = pl.pallas_call(
        functools.partial(kernel, (n, mp, shard, rp, spread, cap)),
        out_shape=(
            jax.ShapeDtypeStruct((shard, kc), F32),
            jax.ShapeDtypeStruct((shard, kc), F32),
            jax.ShapeDtypeStruct((shard, fcol), F32),
            jax.ShapeDtypeStruct((slots, fcol), BF),
        ),
        in_specs=[any_spec] * 7 + [vm] * 5 + [sm] * 2,
        out_specs=(vm, vm, vm, vm),
        scratch_shapes=[
            pltpu.VMEM(x.shape, BF)
            for x in (hidden_rows, key_grad, value_grad, visual_rows)
        ]
        + [
            pltpu.VMEM((slots, width), BF),
            pltpu.VMEM(fc1_weight.shape, BF),
            pltpu.VMEM(fc2_weight.shape, BF),
            pltpu.VMEM((tall, kc), F32),
            pltpu.VMEM((tall, kc), F32),
            pltpu.VMEM((slots // 128, tall, 128), F32),
            pltpu.VMEM((n, rp, slots), BF),
            pltpu.VMEM((n - 1, rp, slots), BF),
        ]
        + stages(na, nb)
        + stages(nb, na)
        + [
            pltpu.VMEM((mp - 1, rows, fcol), BF),
            pltpu.VMEM((mp - 1, rows, fcol), BF),
            pltpu.VMEM((n, slots, fcol), BF),
            dma(7), dma(n - 1), dma(n - 1), dma(mp - 1), dma(mp - 1),
        ]
        + stage_sems(na, nb)
        + stage_sems(nb, na)
        + [dma(n // nc - 1), dma(n // nc - 1), dma(n // nc, nc - 1), dma(n // nc, nc - 1)],
        compiler_params=pltpu.CompilerParams(
            collective_id=0, has_side_effects=True, vmem_limit_bytes=60 * 1024 * 1024
        ),
    )(
        hidden_rows, key_grad, value_grad, visual_rows, visual_cotangent.reshape(slots, width),
        fc1_weight, fc2_weight, norm_gain[None], norm_bias[None], fc1_bias[None], fc2_bias[None],
        layer_scale[None], token_counts, dest_offsets,
    )
    return outs[0], outs[1], outs[2], outs[3].reshape(1, spread, cap, fcol)


def solution(mesh):
    placed = (
        P("dp", None), P("dp", "mp"), P("dp", "mp"), P("dp", None), P("dp", None, None, None),
        P(), P(), P(None, "mp"), P("mp"), P("mp", None), P(), P(), P("dp", None), P("dp", None),
    )
    return jax.shard_map(
        functools.partial(per_device, mesh.shape["dp"], mesh.shape["mp"]),
        mesh=mesh,
        in_specs=placed,
        out_specs=(P("dp", "mp"), P("dp", "mp"), P("dp", "mp"), P("dp", None, None, "mp")),
        check_vma=False,
    )
```

```python
import functools

import jax
import jax.numpy as jnp
from jax import lax
from jax.experimental import pallas as pl
from jax.experimental.pallas import tpu as pltpu
from jax.sharding import PartitionSpec as P

MESH = pl.DeviceIdType.MESH
BF = jnp.bfloat16
F32 = jnp.float32


def up(x, m):
    return -(-x // m) * m


def factors(n):
    core = 2 if n % 2 == 0 else 1
    rest = n // core
    inner = max(f for f in range(1, rest + 1) if rest % f == 0 and f * f <= rest)
    return core, inner, rest // inner


def erf_gelu(x):
    return 0.5 * x * (1.0 + lax.erf(x * (0.5**0.5)))


def kernel(
    cfg,
    hid_h, key_h, val_h, vis_h, cot_h, fc1_h, fc2_h,
    gain, beta, fc1_b, fc2_b, scale, counts, offsets,
    key_o, val_o, proj_o, hand_o,
    hid, key, val, vis, cot, fc1, fc2,
    big_k, big_v, big_c,
    cot_send, cot_recv,
    k0, k0r, k1, k1r, k2, k2r,
    v0, v0r, v1, v1r, v2, v2r,
    z_send, z_recv, gath,
    load_sem, cot_ss, cot_rs, z_ss, z_rs,
    k0_s, k0_r, k1_s, k1_r, k2_s, k2_r,
    v0_s, v0_r, v1_s, v1_r, v2_s, v2_r,
    g_s, g_r, f_s, f_r,
):
    n, mp, shard, rows_pad, spread, cap = cfg
    nc, na, nb = factors(n)
    me = lax.axis_index("dp")
    col = lax.axis_index("mp")
    dc = lax.rem(me, nc)
    da = lax.rem(lax.div(me, nc), na)
    db = lax.div(me, nc * na)
    tokens, width = hid.shape
    slots = cot.shape[0]
    kc = key.shape[1]
    fcol = hand_o.shape[1]

    def rank(c, a, b):
        return (b * na + a) * nc + c

    loads = []
    for i, (src, dst) in enumerate(
        ((cot_h, cot), (vis_h, vis), (fc1_h, fc1), (fc2_h, fc2), (hid_h, hid), (key_h, key), (val_h, val))
    ):
        cp = pltpu.make_async_copy(src, dst, load_sem.at[i])
        cp.start()
        loads.append(cp)
    barrier = pltpu.get_barrier_semaphore()
    for j in range(1, n):
        pl.semaphore_signal(barrier, inc=1, device_id={"dp": lax.rem(me + j, n)}, device_id_type=MESH)
    for j in range(1, mp):
        pl.semaphore_signal(barrier, inc=1, device_id={"mp": lax.rem(col + j, mp)}, device_id_type=MESH)

    def remote(src, dst, ss, rs, where):
        cp = pltpu.make_async_remote_copy(
            src_ref=src, dst_ref=dst, send_sem=ss, recv_sem=rs, device_id=where, device_id_type=MESH
        )
        cp.start()
        return cp

    step = 512 if width % 512 == 0 else 128

    loads[0].wait()
    half = 128

    def turn(i, _):
        at = pl.multiple_of(i * step, step)
        for h in range(slots // half):
            piece = cot[h * half : (h + 1) * half, pl.ds(at, step)].astype(F32)
            big_c[h, pl.ds(at, step), :] = piece.T
        return 0

    lax.fori_loop(0, width // step, turn, 0)
    tail = big_c.shape[1] - width
    big_c[:, width:, :] = jnp.zeros((slots // half, tail, half), F32)
    for r in range(n):
        for h in range(slots // half):
            cot_send[r, :, h * half : (h + 1) * half] = big_c[h, r * shard : r * shard + rows_pad, :].astype(BF)
    pl.semaphore_wait(barrier, n - 1 + mp - 1)
    cot_cps = []

    def send_cot():
        for j in range(1, n):
            to = lax.rem(me + j, n)
            cot_cps.append(remote(cot_send.at[to], cot_recv.at[j - 1], cot_ss.at[j - 1], cot_rs.at[j - 1], {"dp": to}))

    send_cot()

    loads[1].wait()
    values = vis[...].astype(F32)
    center = jnp.mean(values, axis=1, keepdims=True)
    cen = values - center
    var = jnp.mean(cen * cen, axis=1, keepdims=True)
    normed = (cen * lax.rsqrt(var + 1e-06) * gain[...] + beta[...]).astype(BF)
    loads[2].wait()
    hidden = erf_gelu(jnp.dot(normed, fc1[...], preferred_element_type=F32) + fc1_b[...]).astype(BF)
    loads[3].wait()

    def feat(i):
        return pl.ds(pl.multiple_of(i * fcol, 128), fcol)

    z_cps = []
    order = sorted(range(1, mp), key=lambda j: abs(j - mp / 2))
    for j in order:
        to = lax.rem(col + j, mp)
        z_send[j - 1] = jnp.dot(hidden, fc2[:, feat(to)], preferred_element_type=F32).astype(BF)
        z_cps.append(remote(z_send.at[j - 1], z_recv.at[j - 1], z_ss.at[j - 1], z_rs.at[j - 1], {"mp": to}))
    own = jnp.dot(hidden, fc2[:, feat(col)], preferred_element_type=F32)

    for cp in loads[4:]:
        cp.wait()
    kv = jnp.concatenate([key[...], val[...]], axis=1)

    def product(i, _):
        at = pl.multiple_of(i * step, step)
        res = lax.dot_general(hid[:, pl.ds(at, step)], kv, (((0,), (0,)), ((), ())), preferred_element_type=F32)
        big_k[pl.ds(at, step), :] = res[:, :kc]
        big_v[pl.ds(at, step), :] = res[:, kc:]
        return 0

    lax.fori_loop(0, width // step, product, 0)
    first = lax.broadcasted_iota(jnp.int32, (tail, kc), 0) == 0
    big_k[width:, :] = jnp.where(first, jnp.sum(key[...].astype(F32), axis=0, keepdims=True), 0.0)
    big_v[width:, :] = jnp.where(first, jnp.sum(val[...].astype(F32), axis=0, keepdims=True), 0.0)
    for r in range(n):
        c, a, b = r % nc, (r // nc) % na, r // (nc * na)
        k0[c, a, b] = big_k[r * shard : r * shard + rows_pad, :].astype(BF)
        v0[c, b, a] = big_v[r * shard : r * shard + rows_pad, :].astype(BF)

    def exchange(buf, got, ss, rs, digit, q, peer_of):
        cps = []
        for j in range(1, q):
            to = lax.rem(digit + j, q)
            cps.append(remote(buf.at[to], got.at[j - 1], ss.at[j - 1], rs.at[j - 1], {"dp": peer_of(to)}))
        return cps

    def added(buf, got, digit, q, at):
        total = buf[(digit,) + at].astype(F32)
        for j in range(1, q):
            total = total + got[(j - 1,) + at].astype(F32)
        return total

    at_c = lambda c: rank(c, da, db)
    at_a = lambda a: rank(dc, a, db)
    at_b = lambda b: rank(dc, da, b)
    s0k = exchange(k0, k0r, k0_s, k0_r, dc, nc, at_c)
    s0v = exchange(v0, v0r, v0_s, v0_r, dc, nc, at_c)

    rows = vis.shape[0]
    images = counts.shape[1]
    place = lax.broadcasted_iota(jnp.int32, (1, rows), 1)
    target = jnp.full((1, rows), -1, jnp.int32)
    start = jnp.int32(0)
    for i in range(images):
        cnt, off = counts[0, i], offsets[0, i]
        before = jnp.int32(0)
        for e in range(i):
            before = before + jnp.where(offsets[0, e] == off, counts[0, e], 0)
        inside = (place >= start) & (place < start + cnt)
        target = jnp.where(inside, (off - 1) * cap + before + place - start, target)
        start = start + cnt
    slot_id = lax.broadcasted_iota(jnp.int32, (spread * cap, rows), 0)
    select = jnp.where(slot_id == target, 1.0, 0.0).astype(BF)

    for cp in s0k:
        cp.wait_recv()
    for a in range(na):
        for b in range(nb):
            k1[a, b] = added(k0, k0r, dc, nc, (a, b)).astype(BF)
    s1k = exchange(k1, k1r, k1_s, k1_r, da, na, at_a)
    for cp in s0v:
        cp.wait_recv()
    for b in range(nb):
        for a in range(na):
            v1[b, a] = added(v0, v0r, dc, nc, (b, a)).astype(BF)
    s1v = exchange(v1, v1r, v1_s, v1_r, db, nb, at_b)

    for cp in z_cps:
        cp.wait_recv()
    summed = own
    for j in range(1, mp):
        summed = summed + z_recv[j - 1].astype(F32)
    encoded = (
        vis[:, feat(col)].astype(F32) + scale[:, feat(col)] * (summed + fc2_b[:, feat(col)])
    ).astype(BF)
    gath[me] = jnp.dot(select, encoded, preferred_element_type=F32).astype(BF)
    chips = n // nc
    chip = lax.div(me, nc)
    g_cps, f_cps = [], []
    for j in range(1, nc):
        f_cps.append(
            remote(gath.at[me], gath.at[me], f_s.at[0, j - 1], f_r.at[0, j - 1], {"dp": at_c(lax.rem(dc + j, nc))})
        )
    for j in range(1, chips):
        to = lax.rem(chip + j, chips) * nc + dc
        g_cps.append(remote(gath.at[me], gath.at[me], g_s.at[j - 1], g_r.at[j - 1], {"dp": to}))

    for cp in s1k:
        cp.wait_recv()
    for b in range(nb):
        k2[b] = added(k1, k1r, da, na, (b,)).astype(BF)
    s2k = exchange(k2, k2r, k2_s, k2_r, db, nb, at_b)
    for cp in s1v:
        cp.wait_recv()
    for a in range(na):
        v2[a] = added(v1, v1r, db, nb, (a,)).astype(BF)
    s2v = exchange(v2, v2r, v2_s, v2_r, da, na, at_a)

    for j in range(1, chips):
        g_cps[j - 1].wait_recv()
        source = lax.rem(chip + chips - j, chips) * nc + dc
        for i in range(1, nc):
            f_cps.append(
                remote(
                    gath.at[source], gath.at[source], f_s.at[j, i - 1], f_r.at[j, i - 1],
                    {"dp": at_c(lax.rem(dc + i, nc))},
                )
            )
    for cp in f_cps:
        cp.wait_recv()

    def received(r):
        parts = []
        for k in range(1, spread + 1):
            source = lax.rem(r + n - k, n)
            parts.append(gath[source, (k - 1) * cap : k * cap, :])
        return jnp.concatenate(parts, axis=0)

    mine = received(me)
    hand_o[...] = mine
    total = jnp.dot(cot_send[me], mine, preferred_element_type=F32)
    for j in range(1, n):
        cot_cps[j - 1].wait_recv()
        total = total + jnp.dot(
            cot_recv[j - 1], received(lax.rem(me + n - j, n)), preferred_element_type=F32
        )
    proj_o[...] = total[:shard]

    for cp in s2k:
        cp.wait_recv()
    key_o[...] = added(k2, k2r, db, nb, ())[:shard]
    for cp in s2v:
        cp.wait_recv()
    val_o[...] = added(v2, v2r, da, na, ())[:shard]
    for cp in cot_cps + z_cps + s0k + s0v + s1k + s1v + s2k + s2v + g_cps + f_cps:
        cp.wait_send()


def finish(*refs):
    half = len(refs) // 2
    for src, dst in zip(refs[:half], refs[half:]):
        dst[...] = src[...]


def per_device(
    n, mp, hidden_rows, key_grad, value_grad, visual_rows, visual_cotangent, norm_gain, norm_bias,
    fc1_weight, fc1_bias, fc2_weight, fc2_bias, layer_scale, token_counts, dest_offsets,
):
    tokens, width = hidden_rows.shape
    spread, cap = visual_cotangent.shape[1:3]
    slots = spread * cap
    shard = (width + n) // n
    rp = up(shard, 16)
    nc, na, nb = factors(n)
    kc = key_grad.shape[1]
    rows, feats = visual_rows.shape
    fcol = feats // mp
    tall = up(max((n - 1) * shard + rp, width + 8), 8)
    any_spec = pl.BlockSpec(memory_space=pl.ANY)
    vm = pl.BlockSpec(memory_space=pltpu.VMEM)
    sm = pl.BlockSpec(memory_space=pltpu.SMEM)
    dma = lambda *s: pltpu.SemaphoreType.DMA(tuple(max(x, 1) for x in s))

    def stages(q1, q2):
        return [
            pltpu.VMEM((nc, q1, q2, rp, kc), BF),
            pltpu.VMEM((max(nc - 1, 1), q1, q2, rp, kc), BF),
            pltpu.VMEM((q1, q2, rp, kc), BF),
            pltpu.VMEM((max(q1 - 1, 1), q2, rp, kc), BF),
            pltpu.VMEM((q2, rp, kc), BF),
            pltpu.VMEM((max(q2 - 1, 1), rp, kc), BF),
        ]

    def stage_sems(q1, q2):
        return [dma(q - 1) for q in (nc, nc, q1, q1, q2, q2)]

    outs = pl.pallas_call(
        functools.partial(kernel, (n, mp, shard, rp, spread, cap)),
        out_shape=(
            jax.ShapeDtypeStruct((shard, kc), F32),
            jax.ShapeDtypeStruct((shard, kc), F32),
            jax.ShapeDtypeStruct((shard, fcol), F32),
            jax.ShapeDtypeStruct((slots, fcol), BF),
        ),
        in_specs=[any_spec] * 7 + [vm] * 5 + [sm] * 2,
        out_specs=(vm, vm, vm, vm),
        scratch_shapes=[
            pltpu.VMEM(x.shape, BF)
            for x in (hidden_rows, key_grad, value_grad, visual_rows)
        ]
        + [
            pltpu.VMEM((slots, width), BF),
            pltpu.VMEM(fc1_weight.shape, BF),
            pltpu.VMEM(fc2_weight.shape, BF),
            pltpu.VMEM((tall, kc), F32),
            pltpu.VMEM((tall, kc), F32),
            pltpu.VMEM((slots // 128, tall, 128), F32),
            pltpu.VMEM((n, rp, slots), BF),
            pltpu.VMEM((n - 1, rp, slots), BF),
        ]
        + stages(na, nb)
        + stages(nb, na)
        + [
            pltpu.VMEM((mp - 1, rows, fcol), BF),
            pltpu.VMEM((mp - 1, rows, fcol), BF),
            pltpu.VMEM((n, slots, fcol), BF),
            dma(7), dma(n - 1), dma(n - 1), dma(mp - 1), dma(mp - 1),
        ]
        + stage_sems(na, nb)
        + stage_sems(nb, na)
        + [dma(n // nc - 1), dma(n // nc - 1), dma(n // nc, nc - 1), dma(n // nc, nc - 1)],
        compiler_params=pltpu.CompilerParams(
            collective_id=0, has_side_effects=True, vmem_limit_bytes=60 * 1024 * 1024
        ),
    )(
        hidden_rows, key_grad, value_grad, visual_rows, visual_cotangent.reshape(slots, width),
        fc1_weight, fc2_weight, norm_gain[None], norm_bias[None], fc1_bias[None], fc2_bias[None],
        layer_scale[None], token_counts, dest_offsets,
    )
    outs = pl.pallas_call(
        finish,
        out_shape=tuple(jax.ShapeDtypeStruct(x.shape, x.dtype) for x in outs),
        in_specs=[vm] * 4,
        out_specs=(vm,) * 4,
    )(*outs)
    return outs[0], outs[1], outs[2], outs[3].reshape(1, spread, cap, fcol)


def solution(mesh):
    placed = (
        P("dp", None), P("dp", "mp"), P("dp", "mp"), P("dp", None), P("dp", None, None, None),
        P(), P(), P(None, "mp"), P("mp"), P("mp", None), P(), P(), P("dp", None), P("dp", None),
    )
    return jax.shard_map(
        functools.partial(per_device, mesh.shape["dp"], mesh.shape["mp"]),
        mesh=mesh,
        in_specs=placed,
        out_specs=(P("dp", "mp"), P("dp", "mp"), P("dp", "mp"), P("dp", None, None, "mp")),
        check_vma=False,
    )
```
